32 devices in a mesh: slab: 16 (over z, x, core), layer: 2 (over y).
Axes of the slice: x: 2, y: 2, z: 4, core: 2. Of those that a mesh axis runs over, the one named last changes fastest.
Arguments:
- nodal_field: float32 [2, 1024, 4, 4, 512], P('layer', 'slab'), may hold values from -6 to 6
- metric: float32 [2, 1024, 4, 4, 3, 512], P('layer', 'slab'), may hold values from 0.25 to 2
- slab_ids: int32 [1024], replicated, may hold values from 0 to 1023, as said below
- face_map: int32 [1024, 1024], P('slab'), may hold values from 0 to 1023, as said below
Outputs:
- assembled: float32 [2, 1024, 4, 4, 512], P('layer', 'slab')
The draws below stay inside these ranges and needn't reach their ends.
Inputs may be any that keep to these rules, and one draw needn't show every extreme that they name: slab_ids is a permutation of 0 to 1023; positions p of one device are those with p // 64 equal to its index along slab, and for one rotation R every device holds exactly the slabs g with (g + R) mod 16 equal to its index, in any order of its positions, so slab (g + 1) mod 1024 always sits on the next device along slab, cyclically. Each row of face_map is a permutation of 0 to 1023: either the identity, or the map that reverses y, sending (ez, ey, c, b) to (ez, 3 - ey, c, 7 - b); z order is never changed.
All inputs are finite; a program needn't handle non-finite values.
Results may differ from the reference program's by a relative error of at most 0.00005.
Values sent between devices are 32-bit elements; how exact they have to be, the bound alone decides.
No kernel may reach another device: no remote copies, remote signals or barrier semaphores. Data moves between devices by JAX's collectives and lax.ppermute only.
A program may use at most 192 MiB of HBM per device.

```python
import math
import jax
import jax.numpy as jnp
import numpy as np
from jax import lax

P_SIZE = 8
PTS = 512
EY = 4
EZ = 4
SLAB_DEV = 64
FACE = 1024
SLABS = 1024
LAYERS = 2
N_SLAB = 16


def permute_slots(sub_key):
    return jax.random.permutation(sub_key, SLAB_DEV)


def draw_slab_ids(key, part):
    rotate_key = jax.random.fold_in(key, 11)
    order_key = jax.random.fold_in(key, 12)
    rotation = jax.random.randint(rotate_key, (), 0, N_SLAB)
    key_list = jax.random.split(order_key, N_SLAB)
    slot_orders = jax.vmap(permute_slots)(key_list).astype(jnp.int32)
    residues = (jnp.arange(N_SLAB, dtype=jnp.int32) - rotation + N_SLAB) % N_SLAB
    return (slot_orders * N_SLAB + residues[:, None]).reshape(SLABS).astype(jnp.int32)


def draw_face_map(key, part):
    flip_key = jax.random.fold_in(key, 21)
    flip_bits = jax.random.randint(flip_key, (SLABS, 1), 0, 2)
    point_index = jnp.arange(FACE, dtype=jnp.int32)
    column = point_index % P_SIZE
    element_col = point_index // (P_SIZE * P_SIZE) % EY
    reversed_index = point_index + (P_SIZE - 1 - 2 * column) + (EY - 1 - 2 * element_col) * P_SIZE * P_SIZE
    return jnp.where(flip_bits == 1, reversed_index[None, :], point_index[None, :]).astype(jnp.int32)


def steps_of(rng, dims, shards, low, high):
    loudness, own = 1.0, jax.random.fold_in(rng, 6)
    for position, parts in shards:
        steps = jnp.exp(jax.random.uniform(jax.random.fold_in(own, position), (parts,), jnp.float32, low / len(shards), high / len(shards)))
        loudness = loudness * jnp.repeat(steps, dims[position] // parts).reshape([-1 if axis == position else 1 for axis in range(len(dims))])
    return loudness


def noise(key, shape, spread, limit, cuts=(), kind=jnp.bfloat16):
    drawn = spread * jax.random.normal(key, shape, jnp.float32)
    if cuts:
        drawn = drawn * steps_of(key, shape, cuts, -0.22, 0.18)
    return jnp.clip(drawn, -limit, limit).astype(kind)


def setup_inputs(seed: int = 0) -> dict:
    arg_keys = jax.random.split(jax.random.key(seed), 5)
    nodal_field = noise(arg_keys[0], (LAYERS, SLABS, EZ, EY, PTS), 1.0, 6.0, ((0, 2), (1, 16)), jnp.float32)
    metric = jnp.clip(jnp.exp(math.log(2.0) - 2.0794415 * jax.random.uniform(arg_keys[1], (LAYERS, SLABS, EZ, EY, 3, PTS), jnp.float32) ** steps_of(arg_keys[1], (LAYERS, SLABS, EZ, EY, 3, PTS), ((0, 2), (1, 16)), -0.2, 0.2)), 0.25, 2.0)
    slab_ids = draw_slab_ids(jax.random.fold_in(arg_keys[4], 71), 0)
    face_map = draw_face_map(jax.random.fold_in(arg_keys[4], 71), 0)
    return dict(nodal_field=nodal_field, metric=metric, slab_ids=slab_ids, face_map=face_map)


def legendre_pair(gll_nodes, degree):
    lower_poly = gll_nodes * 0.0 + 1.0
    upper_poly = gll_nodes.copy()
    for poly_order in range(2, degree + 1):
        lower_poly, upper_poly = upper_poly, ((2 * poly_order - 1) * gll_nodes * upper_poly - (poly_order - 1) * lower_poly) / poly_order
    return lower_poly, upper_poly


def gll_tables():
    degree = P_SIZE - 1
    gll_nodes = -np.cos(np.pi * np.arange(P_SIZE) / degree)
    for newton_sweep in range(100):
        lower_poly, upper_poly = legendre_pair(gll_nodes, degree)
        gll_nodes = gll_nodes - (gll_nodes * upper_poly - lower_poly) / ((degree + 1) * upper_poly)
    lower_poly, upper_poly = legendre_pair(gll_nodes, degree)
    quad_weights = 2.0 / (degree * (degree + 1) * upper_poly * upper_poly)
    identity = np.eye(P_SIZE)
    differ = gll_nodes[:, None] - gll_nodes[None, :] + identity
    derivative = upper_poly[:, None] / (upper_poly[None, :] * differ)
    derivative = derivative * (1.0 - identity)
    derivative[0, 0] = -degree * (degree + 1) / 4.0
    derivative[degree, degree] = degree * (degree + 1) / 4.0
    weight_cube = quad_weights[:, None, None] * quad_weights[None, :, None] * quad_weights[None, None, :]
    return jnp.asarray(derivative, jnp.float32), jnp.asarray(weight_cube, jnp.float32)


def local_apply(values, factors, derivative, weight_cube):
    highest = lax.Precision.HIGHEST
    grad_x = jnp.einsum("ai,...cbi->...cba", derivative, values, precision=highest)
    grad_y = jnp.einsum("bi,...cia->...cba", derivative, values, precision=highest)
    grad_z = jnp.einsum("ci,...iba->...cba", derivative, values, precision=highest)
    flux_x = weight_cube * factors[..., 0, :, :, :] * grad_x
    flux_y = weight_cube * factors[..., 1, :, :, :] * grad_y
    flux_z = weight_cube * factors[..., 2, :, :, :] * grad_z
    result = jnp.einsum("ia,...cbi->...cba", derivative, flux_x, precision=highest)
    result = result + jnp.einsum("ib,...cia->...cba", derivative, flux_y, precision=highest)
    result = result + jnp.einsum("ic,...iba->...cba", derivative, flux_z, precision=highest)
    return result


def assemble_slab(values):
    shared = values[..., :, :-1, :, P_SIZE - 1, :] + values[..., :, 1:, :, 0, :]
    values = values.at[..., :, :-1, :, P_SIZE - 1, :].set(shared)
    values = values.at[..., :, 1:, :, 0, :].set(shared)
    shared = values[..., :-1, :, P_SIZE - 1, :, :] + values[..., 1:, :, 0, :, :]
    values = values.at[..., :-1, :, P_SIZE - 1, :, :].set(shared)
    values = values.at[..., 1:, :, 0, :, :].set(shared)
    return values


def face_of(local_out, column):
    return local_out[..., column].reshape(local_out.shape[:-5] + (FACE,))


def put_face(local_out, face_values, column):
    return local_out.at[..., column].set(face_values.reshape(local_out.shape[:-1]))


def reference(nodal_field, metric, slab_ids, face_map):
    derivative, weight_cube = gll_tables()
    values = nodal_field.reshape(LAYERS * N_SLAB, SLAB_DEV, EZ, EY, P_SIZE, P_SIZE, P_SIZE)
    factors = metric.reshape(LAYERS * N_SLAB, SLAB_DEV, EZ, EY, 3, P_SIZE, P_SIZE, P_SIZE)

    def slab_block(pair_in):
        return assemble_slab(local_apply(pair_in[0], pair_in[1], derivative, weight_cube))

    local_out = lax.map(slab_block, (values, factors)).reshape(LAYERS, SLABS, EZ, EY, P_SIZE, P_SIZE, P_SIZE)
    slab_iota = jnp.arange(SLABS, dtype=jnp.int32)
    inverse = jnp.zeros((SLABS,), jnp.int32).at[slab_ids].set(slab_iota)
    next_pos = inverse[(slab_ids + 1) % SLABS]
    prev_pos = inverse[(slab_ids + SLABS - 1) % SLABS]
    right_face = face_of(local_out, P_SIZE - 1)
    left_face = face_of(local_out, 0)
    reoriented = jnp.zeros_like(right_face).at[:, slab_iota[:, None], face_map].set(right_face)
    left_sum = left_face + reoriented[:, prev_pos]
    right_sum = right_face + jnp.take_along_axis(left_face[:, next_pos], face_map[None, :, :], axis=2)
    local_out = put_face(local_out, left_sum, 0)
    local_out = put_face(local_out, right_sum, P_SIZE - 1)
    top_face = local_out[:, :, EZ - 1, :, P_SIZE - 1, :, :]
    bottom_face = local_out[:, :, 0, :, 0, :, :]
    top_sum = top_face + jnp.roll(bottom_face, -1, axis=0)
    bottom_sum = bottom_face + jnp.roll(top_face, 1, axis=0)
    local_out = local_out.at[:, :, 0, :, 0, :, :].set(bottom_sum)
    local_out = local_out.at[:, :, EZ - 1, :, P_SIZE - 1, :, :].set(top_sum)
    return local_out.reshape(LAYERS, SLABS, EZ, EY, PTS)
```

```python
import jax
import jax.numpy as jnp
import numpy as np
from jax import lax
from jax.experimental import pallas as pl
from jax.experimental.pallas import tpu as pltpu
from jax.sharding import PartitionSpec as P

P_SIZE = 8
PTS = 512
EY = 4
EZ = 4
TILES = EZ * 2
BLOCK = 8
FIX_BLOCK = 8


def legendre_pair(gll_nodes, degree):
    lower_poly = gll_nodes * 0.0 + 1.0
    upper_poly = gll_nodes.copy()
    for poly_order in range(2, degree + 1):
        lower_poly, upper_poly = (
            upper_poly,
            ((2 * poly_order - 1) * gll_nodes * upper_poly - (poly_order - 1) * lower_poly)
            / poly_order,
        )
    return (lower_poly, upper_poly)


def gll_tables():
    degree = P_SIZE - 1
    gll_nodes = -np.cos(np.pi * np.arange(P_SIZE) / degree)
    for newton_sweep in range(100):
        lower_poly, upper_poly = legendre_pair(gll_nodes, degree)
        gll_nodes = gll_nodes - (gll_nodes * upper_poly - lower_poly) / ((degree + 1) * upper_poly)
    lower_poly, upper_poly = legendre_pair(gll_nodes, degree)
    quad_weights = 2.0 / (degree * (degree + 1) * upper_poly * upper_poly)
    identity = np.eye(P_SIZE)
    differ = gll_nodes[:, None] - gll_nodes[None, :] + identity
    derivative = upper_poly[:, None] / (upper_poly[None, :] * differ)
    derivative = derivative * (1.0 - identity)
    derivative[0, 0] = -degree * (degree + 1) / 4.0
    derivative[degree, degree] = degree * (degree + 1) / 4.0
    return derivative, quad_weights


def split_table(table):
    high = table.astype(np.float32).astype(jnp.bfloat16)
    low = (table - high.astype(np.float64)).astype(np.float32).astype(jnp.bfloat16)
    return high, low


def kernel_tables():
    derivative, rho = gll_tables()
    two = np.eye(2)
    eye = np.eye(P_SIZE)
    plane = np.tile(np.kron(rho, rho), 2)
    along_x = np.kron(two, np.kron(eye, derivative))
    along_y = np.kron(two, np.kron(derivative, eye))
    forward = np.concatenate([along_x.T * plane[None, :], along_y.T * plane[None, :]], 1)
    backward = np.concatenate([along_x, along_y], 0)
    f_high, f_low = split_table(forward)
    b_high, b_low = split_table(backward)
    fwd_a = np.concatenate([f_high, f_high], 0)
    bwd_a = np.concatenate([b_high, b_low], 1)
    sub = np.arange(8)[:, None]
    lane = np.arange(128)[None, :]
    point = lane % 64
    in_plane = rho[point // 8] * rho[point % 8]
    z_fwd = np.zeros((2, 8, 8, 128))
    z_bwd = np.zeros((2, 8, 8, 128))
    rho_c = np.zeros((2, 8, 128))
    for half in range(2):
        c = 4 * half + 2 * (sub // 4) + lane // 64
        rho_c[half] = rho[c]
        for source in range(2):
            for swap_sub in range(2):
                for swap_lane in range(2):
                    other = 4 * source + 2 * (sub // 4 ^ swap_sub) + (lane // 64 ^ swap_lane)
                    k = source * 4 + swap_sub * 2 + swap_lane
                    z_fwd[half, k] = derivative[c, other] * rho[c] * in_plane
                    z_bwd[half, k] = derivative[other, c]
    coeffs = np.concatenate(
        [z_fwd.reshape(16, 8, 128), z_bwd.reshape(16, 8, 128), rho_c], 0
    )
    tables = (fwd_a, f_low, bwd_a, b_high, coeffs.astype(np.float32))
    return tuple(jnp.asarray(table) for table in tables)


def split(value):
    high = value.astype(jnp.bfloat16)
    low = (value - high.astype(jnp.float32)).astype(jnp.bfloat16)
    return high, low


def dot(a, b):
    return jnp.dot(a, b, preferred_element_type=jnp.float32)


def along_z(pair, coeffs, base):
    variants = []
    for value in pair:
        turned = pltpu.roll(value, 64, 1)
        variants += [value, turned, pltpu.roll(value, 4, 0), pltpu.roll(turned, 4, 0)]
    out = []
    for half in range(2):
        terms = [coeffs[base + half * 8 + k] * variants[k] for k in range(8)]
        while len(terms) > 1:
            terms = [terms[i] + terms[i + 1] for i in range(0, len(terms), 2)]
        out.append(terms[0])
    return out


def lanes_from(value, index):
    return jnp.take_along_axis(value, index, axis=1, mode="promise_in_bounds")


def flip(value, sub, lane):
    value = lanes_from(value, lane ^ 7)
    odd = jnp.where(sub % 2 == 0, pltpu.roll(value, 7, 0), pltpu.roll(value, 1, 0))
    return jnp.where(sub % 4 < 2, pltpu.roll(odd, 6, 0), pltpu.roll(odd, 2, 0))


def iotas():
    sub = lax.broadcasted_iota(jnp.int32, (8, 128), 0)
    lane = lax.broadcasted_iota(jnp.int32, (8, 128), 1)
    return sub, lane


def turned_flag(map_ref, row):
    return jnp.broadcast_to(map_ref[pl.ds(row, 1), 0:1], (8, 128)) != 0


def apply_kernel(
    u_ref, m_ref, map_ref, fa_ref, fl_ref, ba_ref, bh_ref, co_ref,
    out_ref, left_ref, right_ref, zed_ref, el_ref, er_ref,
    g_ref, fh_ref, fl2_ref, lz_ref, l_ref,
):
    step = pl.program_id(0)
    sub, lane = iotas()
    rows = u_ref.shape[0]
    slabs = rows // 64
    u = u_ref[...].reshape(slabs * EZ, 2, 8, 128)
    v = (u * co_ref[32:34][None]).reshape(rows, 128)
    high, low = split(v)
    uk = jnp.concatenate([high, low], 1)
    g_ref[...] = dot(uk, fa_ref[...]) + dot(high, fl_ref[...])

    for e in range(slabs * EZ):
        base = e * 16
        mbase = e * 48
        pair = [u_ref[base : base + 8, :], u_ref[base + 8 : base + 16, :]]
        grad = along_z(pair, co_ref, 0)
        flux = [
            grad[h] * m_ref[mbase + 32 + 8 * h : mbase + 40 + 8 * h, :] for h in range(2)
        ]
        back = along_z(flux, co_ref, 16)
        for h in range(2):
            lz_ref[base + 8 * h : base + 8 * h + 8, :] = back[h]
        fx = m_ref[mbase : mbase + 16, :] * g_ref[base : base + 16, :128]
        fy = m_ref[mbase + 16 : mbase + 32, :] * g_ref[base : base + 16, 128:]
        xh, xl = split(fx)
        yh, yl = split(fy)
        fh_ref[base : base + 16, :128] = xh
        fh_ref[base : base + 16, 128:] = yh
        fl2_ref[base : base + 16, :128] = xl
        fl2_ref[base : base + 16, 128:] = yl
    both = dot(fh_ref[...], ba_ref[...])
    l_ref[...] = both[:, :128] + both[:, 128:] + dot(fl2_ref[...], bh_ref[...]) + lz_ref[...]

    b = lane // 8 % 8
    ey = sub % 4
    after_mask = (b == 7) & (ey < 3)
    before_mask = (b == 0) & (ey > 0)
    high_c = (sub >= 4) & (lane >= 64)
    low_c = (sub < 4) & (lane < 64)
    index_left = lane % 16 * 8
    index_right = index_left + 7
    slot = lane // 16
    slot8 = lane // 8
    for s in range(slabs):
        tiles = []
        for k in range(TILES):
            row = s * 64 + k * 8
            t = l_ref[row : row + 8, :]
            after = pltpu.roll(pltpu.roll(t, 56, 1), 7, 0)
            before = pltpu.roll(pltpu.roll(t, 72, 1), 1, 0)
            tiles.append(
                t + jnp.where(after_mask, after, 0.0) + jnp.where(before_mask, before, 0.0)
            )
        for e in range(EZ - 1):
            top = tiles[2 * e + 1]
            bottom = tiles[2 * e + 2]
            tiles[2 * e + 1] = top + jnp.where(
                high_c, pltpu.roll(pltpu.roll(bottom, 64, 1), 4, 0), 0.0
            )
            tiles[2 * e + 2] = bottom + jnp.where(
                low_c, pltpu.roll(pltpu.roll(top, 64, 1), 4, 0), 0.0
            )
        left = jnp.zeros((8, 128), jnp.float32)
        right = left
        for k in range(TILES):
            row = s * 64 + k * 8
            out_ref[row : row + 8, :] = tiles[k]
            left = jnp.where(slot == k, lanes_from(tiles[k], index_left), left)
            right = jnp.where(slot == k, lanes_from(tiles[k], index_right), right)
        flag = turned_flag(map_ref, step * slabs + s)
        right = jnp.where(flag, flip(right, sub, lane), right)
        left_ref[s * 8 : s * 8 + 8, :] = left
        right_ref[s * 8 : s * 8 + 8, :] = right
        zed = jnp.where(sub < 4, tiles[0], tiles[TILES - 1])
        if s % 2 == 0:
            even = zed
        else:
            odd = pltpu.roll(zed, 64, 1)
            zed_ref[s // 2 * 8 : s // 2 * 8 + 8, :] = jnp.where(
                (sub < 4) == (lane < 64), even, odd
            )
        place = step * slabs + s
        place16 = place % 16
        mask = ((slot8 == place16) & (sub < 4)) | (
            (slot8 == (place16 + 15) % 16) & (sub >= 4)
        )
        if s == 0:
            acc_l = jnp.zeros((8, 128), jnp.float32)
            acc_r = acc_l
        acc_l = jnp.where(mask, pltpu.roll(left, place16 * 8, 1), acc_l)
        acc_r = jnp.where(mask, pltpu.roll(right, place16 * 8, 1), acc_r)
    per = 16 // slabs
    first = step % per == 0
    where = pl.ds(pl.multiple_of(step // per * 8, 8), 8)
    el_ref[where, :] = jnp.where(first, acc_l, el_ref[where, :] + acc_l)
    er_ref[where, :] = jnp.where(first, acc_r, er_ref[where, :] + acc_r)


def fix_kernel(
    prev_ref, next_ref, in_ref, map_ref, fprev_ref, fnext_ref, zed_ref, eprev_ref, enext_ref,
    out_ref,
):
    step = pl.program_id(0)
    sub, lane = iotas()
    slabs = in_ref.shape[0] // 64
    a = lane % 8
    low_c = (sub < 4) & (lane < 64)
    high_c = (sub >= 4) & (lane >= 64)
    low_edge = (sub < 4) & (lane < 8)
    high_edge = (sub >= 4) & (lane >= 120)

    def incoming(face_ref, edge_ref, j):
        face = face_ref[pl.ds(pl.multiple_of(j * 8, 8), 8), :]
        edge = edge_ref[pl.ds(pl.multiple_of(j // 16 * 8, 8), 8), :]
        shift = (16 - j % 16) % 16 * 8
        edge = pltpu.roll(pltpu.roll(edge, shift, 1), 4, 0)
        edge = jnp.where(
            low_edge,
            pltpu.roll(edge, 8, 1),
            jnp.where(high_edge, pltpu.roll(edge, 120, 1), 0.0),
        )
        return face + edge

    for s in range(slabs):
        p = step * slabs + s
        left = incoming(fprev_ref, eprev_ref, prev_ref[p])
        right = incoming(fnext_ref, enext_ref, next_ref[p])
        right = jnp.where(turned_flag(map_ref, p), flip(right, sub, lane), right)
        zed = pltpu.roll(zed_ref[s // 2 * 8 : s // 2 * 8 + 8, :], 4, 0)
        if s % 2 == 0:
            zed = pltpu.roll(zed, 64, 1)
        for k in range(TILES):
            row = s * 64 + k * 8
            index = k * 16 + lane // 8
            t = in_ref[row : row + 8, :]
            t = t + jnp.where(a == 0, lanes_from(left, index), 0.0)
            t = t + jnp.where(a == 7, lanes_from(right, index), 0.0)
            if k == 0:
                t = t + jnp.where(low_c, zed, 0.0)
            if k == TILES - 1:
                t = t + jnp.where(high_c, zed, 0.0)
            out_ref[row : row + 8, :] = t


def whole_of(array):
    return pl.BlockSpec(array.shape, lambda i, *_: (0,) * array.ndim)


def apply_local(u, m, face_map, tables, slab_count):
    steps = slab_count // BLOCK
    rows = BLOCK * 64
    f32 = jnp.float32
    shapes = [
        (slab_count * 64, 128),
        (slab_count * 8, 128),
        (slab_count * 8, 128),
        (slab_count * 4, 128),
        (slab_count // 2, 128),
        (slab_count // 2, 128),
    ]
    row_block = lambda n: pl.BlockSpec((n, 128), lambda i: (i, 0))
    return pl.pallas_call(
        apply_kernel,
        grid=(steps,),
        in_specs=[
            row_block(rows),
            row_block(rows * 3),
            pl.BlockSpec((slab_count, 128), lambda i: (0, 0)),
        ]
        + [whole_of(t) for t in tables],
        out_specs=[
            row_block(rows),
            row_block(BLOCK * 8),
            row_block(BLOCK * 8),
            row_block(BLOCK * 4),
            pl.BlockSpec(shapes[4], lambda i: (0, 0)),
            pl.BlockSpec(shapes[5], lambda i: (0, 0)),
        ],
        out_shape=[jax.ShapeDtypeStruct(s, f32) for s in shapes],
        scratch_shapes=[
            pltpu.VMEM((rows, 256), f32),
            pltpu.VMEM((rows, 256), jnp.bfloat16),
            pltpu.VMEM((rows, 256), jnp.bfloat16),
            pltpu.VMEM((rows, 128), f32),
            pltpu.VMEM((rows, 128), f32),
        ],
        name="apply_local",
    )(u, m, face_map, *tables)


def fix_faces(prev_index, next_index, local, face_map, fprev, fnext, zed, eprev, enext):
    slab_count = face_map.shape[0]
    steps = slab_count // FIX_BLOCK
    rows = FIX_BLOCK * 64
    return pl.pallas_call(
        fix_kernel,
        grid_spec=pltpu.PrefetchScalarGridSpec(
            num_scalar_prefetch=2,
            grid=(steps,),
            in_specs=[
                pl.BlockSpec((rows, 128), lambda i, *_: (i, 0)),
                pl.BlockSpec((slab_count, 128), lambda i, *_: (0, 0)),
                whole_of(fprev),
                whole_of(fnext),
                pl.BlockSpec((FIX_BLOCK * 4, 128), lambda i, *_: (i, 0)),
                whole_of(eprev),
                whole_of(enext),
            ],
            out_specs=pl.BlockSpec((rows, 128), lambda i, *_: (i, 0)),
        ),
        out_shape=jax.ShapeDtypeStruct(local.shape, jnp.float32),
        name="fix_faces",
    )(prev_index, next_index, local, face_map, fprev, fnext, zed, eprev, enext)


def send(value, by, across):
    slabs = lax.axis_size("slab")
    layers = lax.axis_size("layer")
    pairs = [
        (s * layers + l, (s + by) % slabs * layers + (l + across) % layers)
        for s in range(slabs)
        for l in range(layers)
    ]
    return lax.ppermute(value, ("slab", "layer"), pairs)


def body(nodal_field, metric, slab_ids, face_map):
    slab_count = nodal_field.shape[1]
    cycle_size = lax.axis_size("slab")
    total_slabs = slab_count * cycle_size
    device = lax.axis_index("slab")
    u = nodal_field.reshape(slab_count, EZ, EY, 4, 128).transpose(0, 1, 3, 2, 4)
    u = u.reshape(slab_count * 64, 128)
    m = metric.reshape(slab_count, EZ, EY, 3, 4, 128).transpose(0, 1, 3, 4, 2, 5)
    m = m.reshape(slab_count * 192, 128)
    local, left, right, zed, edge_left, edge_right = apply_local(
        u, m, face_map, kernel_tables(), slab_count
    )
    zed = send(zed, 0, 1)
    fprev = send(right, 1, 0)
    fnext = send(left, -1, 0)
    eprev = send(edge_right, 1, 1)
    enext = send(edge_left, -1, 1)

    def ids_of(index):
        return lax.dynamic_slice_in_dim(slab_ids, index % cycle_size * slab_count, slab_count)

    own_ids = ids_of(device)
    position = jnp.arange(slab_count, dtype=jnp.int32)[None, :]

    def index_of(there, wanted):
        hit = there[None, :] == wanted[:, None]
        return jnp.sum(jnp.where(hit, position, 0), axis=1)

    prev_index = index_of(
        ids_of(device + cycle_size - 1), (own_ids + total_slabs - 1) % total_slabs
    )
    next_index = index_of(ids_of(device + 1), (own_ids + 1) % total_slabs)
    out = fix_faces(prev_index, next_index, local, face_map, fprev, fnext, zed, eprev, enext)
    out = out.reshape(slab_count, EZ, 4, EY, 128).transpose(0, 1, 3, 2, 4)
    return out.reshape(1, slab_count, EZ, EY, PTS)


def solution(mesh):
    return jax.shard_map(
        body,
        mesh=mesh,
        in_specs=(
            P("layer", "slab", None, None, None),
            P("layer", "slab", None, None, None, None),
            P(),
            P("slab", None),
        ),
        out_specs=P("layer", "slab", None, None, None),
        check_vma=False,
    )
```

```python
import functools

import jax
import jax.numpy as jnp
import numpy as np
from jax import lax
from jax.experimental import pallas as pl
from jax.experimental.pallas import tpu as pltpu
from jax.sharding import PartitionSpec as P

P_SIZE = 8
PTS = 512
EY = 4
EZ = 4
TILES = EZ * 2
BLOCK = 8
FIX_BLOCK = 16


def legendre_pair(gll_nodes, degree):
    lower_poly = gll_nodes * 0.0 + 1.0
    upper_poly = gll_nodes.copy()
    for poly_order in range(2, degree + 1):
        lower_poly, upper_poly = (
            upper_poly,
            ((2 * poly_order - 1) * gll_nodes * upper_poly - (poly_order - 1) * lower_poly)
            / poly_order,
        )
    return (lower_poly, upper_poly)


def gll_tables():
    degree = P_SIZE - 1
    gll_nodes = -np.cos(np.pi * np.arange(P_SIZE) / degree)
    for newton_sweep in range(100):
        lower_poly, upper_poly = legendre_pair(gll_nodes, degree)
        gll_nodes = gll_nodes - (gll_nodes * upper_poly - lower_poly) / ((degree + 1) * upper_poly)
    lower_poly, upper_poly = legendre_pair(gll_nodes, degree)
    quad_weights = 2.0 / (degree * (degree + 1) * upper_poly * upper_poly)
    identity = np.eye(P_SIZE)
    differ = gll_nodes[:, None] - gll_nodes[None, :] + identity
    derivative = upper_poly[:, None] / (upper_poly[None, :] * differ)
    derivative = derivative * (1.0 - identity)
    derivative[0, 0] = -degree * (degree + 1) / 4.0
    derivative[degree, degree] = degree * (degree + 1) / 4.0
    return derivative, quad_weights


def split_table(table):
    high = table.astype(np.float32).astype(jnp.bfloat16)
    low = (table - high.astype(np.float64)).astype(np.float32).astype(jnp.bfloat16)
    return high, low


def kernel_tables():
    derivative, rho = gll_tables()
    two = np.eye(2)
    eye = np.eye(P_SIZE)
    plane = np.tile(np.kron(rho, rho), 2)
    along_x = np.kron(two, np.kron(eye, derivative))
    along_y = np.kron(two, np.kron(derivative, eye))
    forward = np.concatenate([along_x.T * plane[None, :], along_y.T * plane[None, :]], 1)
    backward = np.concatenate([along_x, along_y], 0)
    f_high, f_low = split_table(forward)
    b_high, b_low = split_table(backward)
    fwd_a = np.concatenate([f_high, f_high], 0)
    bwd_a = np.concatenate([b_high, b_low], 1)
    sub = np.arange(8)[:, None]
    lane = np.arange(128)[None, :]
    point = lane % 64
    in_plane = rho[point // 8] * rho[point % 8]
    rho_c = np.zeros((2, 8, 128))
    for half in range(2):
        rho_c[half] = rho[4 * half + 2 * (sub // 4) + lane // 64]
    c = 2 * (sub // 4) + lane // 64
    parts = []
    for operator, scale in ((derivative, rho_c[0] * in_plane), (derivative.T, 1.0)):
        for sign in (1, -1):
            for swap in range(4):
                near = operator[c, c ^ swap]
                far = operator[c, 7 - (c ^ swap)]
                parts.append((near + sign * far) * 0.5 * scale)
    coeffs = np.concatenate([np.stack(parts), rho_c], 0)
    lane_in = np.arange(128)[:, None]
    lane_out = np.arange(128)[None, :]
    sides = [lane_in == lane_out % 16 * 8 + edge for edge in (0, 7)]
    pick = np.concatenate(sides, 1).astype(jnp.bfloat16)
    pick = np.concatenate([pick, pick], 0)
    wide = np.arange(TILES * 128)[None, :]
    slot = wide // 128 * 16 + wide % 128 // 8
    spread = [(lane_in == slot) & (wide % 8 == edge) for edge in (0, 7)]
    spread = np.concatenate(spread, 0).astype(jnp.bfloat16)
    tables = (fwd_a, f_low, bwd_a, b_high, coeffs.astype(np.float32), pick)
    return tuple(jnp.asarray(table) for table in tables), jnp.asarray(spread)


def split(value):
    high = value.astype(jnp.bfloat16)
    return high, (value - high.astype(jnp.float32)).astype(jnp.bfloat16)


def dot(a, b):
    return jnp.dot(a, b, preferred_element_type=jnp.float32)


def mirror(value):
    return pltpu.roll(pltpu.roll(value, 64, 1), 4, 0)


def along_z(low, high, coeffs, base):
    sums = []
    for value in (low + high, low - high):
        turned = pltpu.roll(value, 64, 1)
        variants = [value, turned, pltpu.roll(value, 4, 0), pltpu.roll(turned, 4, 0)]
        terms = [coeffs[base + k] * variants[k] for k in range(4)]
        sums.append((terms[0] + terms[1]) + (terms[2] + terms[3]))
        base += 4
    return sums[0] + sums[1], sums[1] - sums[0]


def rank_of(slab, cycle):
    if cycle & (cycle - 1) == 0:
        return slab >> (cycle.bit_length() - 1)
    return lax.div(slab, cycle)


def lanes_from(value, index):
    return jnp.take_along_axis(value, index, axis=1, mode="promise_in_bounds")


def flip(value, sub, lane):
    value = lanes_from(value, lane ^ 7)
    odd = jnp.where(sub % 2 == 0, pltpu.roll(value, 7, 0), pltpu.roll(value, 1, 0))
    return jnp.where(sub % 4 < 2, pltpu.roll(odd, 6, 0), pltpu.roll(odd, 2, 0))


def iotas():
    sub = lax.broadcasted_iota(jnp.int32, (8, 128), 0)
    lane = lax.broadcasted_iota(jnp.int32, (8, 128), 1)
    return sub, lane


def turned_flag(map_ref, row):
    return jnp.broadcast_to(map_ref[pl.ds(row, 1), 0:1], (8, 128)) != 0


def apply_kernel(
    cycle, ids_ref, dev_ref,
    u_ref, m_ref, map_ref, fa_ref, fl_ref, ba_ref, bh_ref, co_ref, pick_ref,
    out_ref, left_ref, right_ref, zed_ref, el_ref, er_ref,
    g_ref, fh_ref, fl2_ref, lz_ref, l_ref, face_ref, pl_ref, pr_ref,
):
    step = pl.program_id(0)
    sub, lane = iotas()
    rows = u_ref.shape[0]
    slabs = rows // 64
    u = u_ref[...].reshape(slabs * EZ, 2, 8, 128)
    v = (u * co_ref[16:18][None]).reshape(rows, 128)
    high, low = split(v)
    uk = jnp.concatenate([high, low], 1)
    g_ref[...] = dot(uk, fa_ref[...]) + dot(high, fl_ref[...])

    for e in range(slabs * EZ):
        base = e * 16
        mbase = e * 48
        low, high = along_z(
            u_ref[base : base + 8, :], mirror(u_ref[base + 8 : base + 16, :]), co_ref, 0
        )
        low = low * m_ref[mbase + 32 : mbase + 40, :]
        high = high * mirror(m_ref[mbase + 40 : mbase + 48, :])
        low, high = along_z(low, high, co_ref, 8)
        lz_ref[base : base + 8, :] = low
        lz_ref[base + 8 : base + 16, :] = mirror(high)
        fx = m_ref[mbase : mbase + 16, :] * g_ref[base : base + 16, :128]
        fy = m_ref[mbase + 16 : mbase + 32, :] * g_ref[base : base + 16, 128:]
        xh, xl = split(fx)
        yh, yl = split(fy)
        fh_ref[base : base + 16, :128] = xh
        fh_ref[base : base + 16, 128:] = yh
        fl2_ref[base : base + 16, :128] = xl
        fl2_ref[base : base + 16, 128:] = yl
    both = dot(fh_ref[...], ba_ref[...])
    l_ref[...] = both[:, :128] + both[:, 128:] + dot(fl2_ref[...], bh_ref[...]) + lz_ref[...]

    b = lane // 8 % 8
    ey = sub % 4
    after_mask = (b == 7) & (ey < 3)
    before_mask = (b == 0) & (ey > 0)
    high_c = (sub >= 4) & (lane >= 64)
    low_c = (sub < 4) & (lane < 64)
    slot = lane // 16
    slot8 = lane // 8
    for s in range(slabs):
        tiles = []
        for k in range(TILES):
            row = s * 64 + k * 8
            t = l_ref[row : row + 8, :]
            after = pltpu.roll(pltpu.roll(t, 56, 1), 7, 0)
            before = pltpu.roll(pltpu.roll(t, 72, 1), 1, 0)
            tiles.append(
                t + jnp.where(after_mask, after, 0.0) + jnp.where(before_mask, before, 0.0)
            )
        for e in range(EZ - 1):
            top = tiles[2 * e + 1]
            bottom = tiles[2 * e + 2]
            tiles[2 * e + 1] = top + jnp.where(
                high_c, pltpu.roll(pltpu.roll(bottom, 64, 1), 4, 0), 0.0
            )
            tiles[2 * e + 2] = bottom + jnp.where(
                low_c, pltpu.roll(pltpu.roll(top, 64, 1), 4, 0), 0.0
            )
        for k in range(TILES):
            row = s * 64 + k * 8
            out_ref[row : row + 8, :] = tiles[k]
        zed = jnp.where(sub < 4, tiles[0], tiles[TILES - 1])
        if s % 2 == 0:
            even = zed
        else:
            odd = pltpu.roll(zed, 64, 1)
            zed_ref[s // 2 * 8 : s // 2 * 8 + 8, :] = jnp.where(
                (sub < 4) == (lane < 64), even, odd
            )
    high, low = split(out_ref[...])
    face_ref[...] = dot(jnp.concatenate([high, low], 1), pick_ref[...])
    for s in range(slabs):
        row = s * 64
        left = face_ref[row : row + 8, :128]
        right = face_ref[row : row + 8, 128:]
        for k in range(1, TILES):
            row = s * 64 + k * 8
            left = jnp.where(slot == k, face_ref[row : row + 8, :128], left)
            right = jnp.where(slot == k, face_ref[row : row + 8, 128:], right)
        position = step * slabs + s
        flag = turned_flag(map_ref, position)
        right = jnp.where(flag, flip(right, sub, lane), right)
        rank = rank_of(ids_ref[dev_ref[0] + position], cycle)
        where = pl.ds(pl.multiple_of(rank * 8, 8), 8)
        left_ref[where, :] = left
        right_ref[where, :] = right
        place = rank & 15
        mask = ((slot8 == place) & (sub < 4)) | ((slot8 == ((place + 15) & 15)) & (sub >= 4))
        pl_ref[where, :] = jnp.where(mask, pltpu.roll(left, place * 8, 1), 0.0)
        pr_ref[where, :] = jnp.where(mask, pltpu.roll(right, place * 8, 1), 0.0)

    @pl.when(step == pl.num_programs(0) - 1)
    def _():
        for from_ref, to_ref in ((pl_ref, el_ref), (pr_ref, er_ref)):
            parts = from_ref[...].reshape(-1, 16, 8, 128)
            to_ref[...] = jnp.sum(parts, axis=1).reshape(to_ref.shape)


def fix_kernel(
    cycle, total, ids_ref, dev_ref,
    in_ref, map_ref, fprev_ref, fnext_ref, zed_ref, eprev_ref, enext_ref, spread_ref,
    out_ref, x_ref, y_ref,
):
    step = pl.program_id(0)
    sub, lane = iotas()
    slabs = in_ref.shape[0] // 64
    low_c = (sub < 4) & (lane < 64)
    high_c = (sub >= 4) & (lane >= 64)
    low_edge = (sub < 4) & (lane < 8)
    high_edge = (sub >= 4) & (lane >= 120)

    def incoming(face_ref, edge_ref, j):
        face = face_ref[pl.ds(pl.multiple_of(j * 8, 8), 8), :]
        edge = edge_ref[pl.ds(pl.multiple_of((j >> 4) * 8, 8), 8), :]
        shift = ((16 - (j & 15)) & 15) * 8
        edge = pltpu.roll(pltpu.roll(edge, shift, 1), 4, 0)
        edge = jnp.where(
            low_edge,
            pltpu.roll(edge, 8, 1),
            jnp.where(high_edge, pltpu.roll(edge, 120, 1), 0.0),
        )
        return face + edge

    half = slabs * 8
    for s in range(slabs):
        p = step * slabs + s
        own = ids_ref[dev_ref[0] + p]
        before = jnp.where(own == 0, total - 1, own - 1)
        after = jnp.where(own == total - 1, 0, own + 1)
        left = incoming(fprev_ref, eprev_ref, rank_of(before, cycle))
        right = incoming(fnext_ref, enext_ref, rank_of(after, cycle))
        right = jnp.where(turned_flag(map_ref, p), flip(right, sub, lane), right)
        x_ref[s * 8 : s * 8 + 8, :128] = left
        x_ref[s * 8 : s * 8 + 8, 128:] = right
    high, low = split(x_ref[...])
    both = dot(jnp.concatenate([high, low], 0), spread_ref[...])
    y_ref[...] = both[:half] + both[half:]
    for s in range(slabs):
        zed = pltpu.roll(zed_ref[s // 2 * 8 : s // 2 * 8 + 8, :], 4, 0)
        if s % 2 == 0:
            zed = pltpu.roll(zed, 64, 1)
        for k in range(TILES):
            row = s * 64 + k * 8
            t = in_ref[row : row + 8, :] + y_ref[s * 8 : s * 8 + 8, k * 128 : k * 128 + 128]
            if k == 0:
                t = t + jnp.where(low_c, zed, 0.0)
            if k == TILES - 1:
                t = t + jnp.where(high_c, zed, 0.0)
            out_ref[row : row + 8, :] = t


def whole_of(array):
    return pl.BlockSpec(array.shape, lambda i, *_: (0,) * array.ndim)


def apply_local(ids, dev, u, m, face_map, tables, cycle):
    slab_count = face_map.shape[0]
    steps = slab_count // BLOCK
    rows = BLOCK * 64
    f32 = jnp.float32
    shapes = [
        (slab_count * 64, 128),
        (slab_count * 8, 128),
        (slab_count * 8, 128),
        (slab_count * 4, 128),
        (slab_count // 2, 128),
        (slab_count // 2, 128),
    ]
    row_block = lambda n: pl.BlockSpec((n, 128), lambda i, *_: (i, 0))
    whole = lambda shape: pl.BlockSpec(shape, lambda i, *_: (0, 0))
    return pl.pallas_call(
        functools.partial(apply_kernel, cycle),
        grid_spec=pltpu.PrefetchScalarGridSpec(
            num_scalar_prefetch=2,
            grid=(steps,),
            in_specs=[row_block(rows), row_block(rows * 3), whole((slab_count, 128))]
            + [whole_of(t) for t in tables],
            out_specs=[
                row_block(rows),
                whole(shapes[1]),
                whole(shapes[2]),
                row_block(BLOCK * 4),
                whole(shapes[4]),
                whole(shapes[5]),
            ],
            scratch_shapes=[
                pltpu.VMEM((rows, 256), f32),
                pltpu.VMEM((rows, 256), jnp.bfloat16),
                pltpu.VMEM((rows, 256), jnp.bfloat16),
                pltpu.VMEM((rows, 128), f32),
                pltpu.VMEM((rows, 128), f32),
                pltpu.VMEM((rows, 256), f32),
                pltpu.VMEM(shapes[1], f32),
                pltpu.VMEM(shapes[1], f32),
            ],
        ),
        out_shape=[jax.ShapeDtypeStruct(s, f32) for s in shapes],
        name="apply_local",
    )(ids, dev, u, m, face_map, *tables)


def fix_faces(ids, dev, local, face_map, fprev, fnext, zed, eprev, enext, spread, cycle):
    slab_count = face_map.shape[0]
    steps = slab_count // FIX_BLOCK
    rows = FIX_BLOCK * 64
    return pl.pallas_call(
        functools.partial(fix_kernel, cycle, slab_count * cycle),
        grid_spec=pltpu.PrefetchScalarGridSpec(
            num_scalar_prefetch=2,
            grid=(steps,),
            in_specs=[
                pl.BlockSpec((rows, 128), lambda i, *_: (i, 0)),
                pl.BlockSpec((slab_count, 128), lambda i, *_: (0, 0)),
                whole_of(fprev),
                whole_of(fnext),
                pl.BlockSpec((FIX_BLOCK * 4, 128), lambda i, *_: (i, 0)),
                whole_of(eprev),
                whole_of(enext),
                whole_of(spread),
            ],
            out_specs=pl.BlockSpec((rows, 128), lambda i, *_: (i, 0)),
            scratch_shapes=[
                pltpu.VMEM((FIX_BLOCK * 8, 256), jnp.float32),
                pltpu.VMEM((FIX_BLOCK * 8, TILES * 128), jnp.float32),
            ],
        ),
        out_shape=jax.ShapeDtypeStruct(local.shape, jnp.float32),
        name="fix_faces",
    )(ids, dev, local, face_map, fprev, fnext, zed, eprev, enext, spread)


def send(value, by, across):
    slabs = lax.axis_size("slab")
    layers = lax.axis_size("layer")
    pairs = [
        (s * layers + l, (s + by) % slabs * layers + (l + across) % layers)
        for s in range(slabs)
        for l in range(layers)
    ]
    return lax.ppermute(value, ("slab", "layer"), pairs)


def body(nodal_field, metric, slab_ids, face_map):
    slab_count = nodal_field.shape[1]
    cycle_size = lax.axis_size("slab")
    first = lax.axis_index("slab").reshape(1) * slab_count
    tables, spread = kernel_tables()
    u = nodal_field.reshape(slab_count, EZ, EY, 4, 128).transpose(0, 1, 3, 2, 4)
    u = u.reshape(slab_count * 64, 128)
    m = metric.reshape(slab_count, EZ, EY, 3, 4, 128).transpose(0, 1, 3, 4, 2, 5)
    m = m.reshape(slab_count * 192, 128)
    local, left, right, zed, edge_left, edge_right = apply_local(
        slab_ids, first, u, m, face_map, tables, cycle_size
    )
    zed = send(zed, 0, 1)
    fprev = send(right, 1, 0)
    fnext = send(left, -1, 0)
    eprev = send(edge_right, 1, 1)
    enext = send(edge_left, -1, 1)

    out = fix_faces(
        slab_ids, first, local, face_map, fprev, fnext, zed, eprev, enext, spread, cycle_size
    )
    out = out.reshape(slab_count, EZ, 4, EY, 128).transpose(0, 1, 3, 2, 4)
    return out.reshape(1, slab_count, EZ, EY, PTS)


def solution(mesh):
    return jax.shard_map(
        body,
        mesh=mesh,
        in_specs=(
            P("layer", "slab", None, None, None),
            P("layer", "slab", None, None, None, None),
            P(),
            P("slab", None),
        ),
        out_specs=P("layer", "slab", None, None, None),
        check_vma=False,
    )
```

```python
import functools

import jax
import jax.numpy as jnp
import numpy as np
from jax import lax
from jax.experimental import pallas as pl
from jax.experimental.pallas import tpu as pltpu
from jax.sharding import PartitionSpec as P

P_SIZE = 8
PTS = 512
EY = 4
EZ = 4
TILES = EZ * 2
BLOCK = 8
FIX_BLOCK = 16


def legendre_pair(gll_nodes, degree):
    lower_poly = gll_nodes * 0.0 + 1.0
    upper_poly = gll_nodes.copy()
    for poly_order in range(2, degree + 1):
        lower_poly, upper_poly = (
            upper_poly,
            ((2 * poly_order - 1) * gll_nodes * upper_poly - (poly_order - 1) * lower_poly)
            / poly_order,
        )
    return (lower_poly, upper_poly)


def gll_tables():
    degree = P_SIZE - 1
    gll_nodes = -np.cos(np.pi * np.arange(P_SIZE) / degree)
    for newton_sweep in range(100):
        lower_poly, upper_poly = legendre_pair(gll_nodes, degree)
        gll_nodes = gll_nodes - (gll_nodes * upper_poly - lower_poly) / ((degree + 1) * upper_poly)
    lower_poly, upper_poly = legendre_pair(gll_nodes, degree)
    quad_weights = 2.0 / (degree * (degree + 1) * upper_poly * upper_poly)
    identity = np.eye(P_SIZE)
    differ = gll_nodes[:, None] - gll_nodes[None, :] + identity
    derivative = upper_poly[:, None] / (upper_poly[None, :] * differ)
    derivative = derivative * (1.0 - identity)
    derivative[0, 0] = -degree * (degree + 1) / 4.0
    derivative[degree, degree] = degree * (degree + 1) / 4.0
    return derivative, quad_weights


def split_table(table):
    high = table.astype(np.float32).astype(jnp.bfloat16)
    low = (table - high.astype(np.float64)).astype(np.float32).astype(jnp.bfloat16)
    return high, low


def kernel_tables():
    derivative, rho = gll_tables()
    two = np.eye(2)
    eye = np.eye(P_SIZE)
    plane = np.tile(np.kron(rho, rho), 2)
    along_x = np.kron(two, np.kron(eye, derivative))
    along_y = np.kron(two, np.kron(derivative, eye))
    forward = np.concatenate([along_x.T * plane[None, :], along_y.T * plane[None, :]], 1)
    backward = np.concatenate([along_x, along_y], 0)
    f_high, f_low = split_table(forward)
    b_high, b_low = split_table(backward)
    fwd_a = np.concatenate([f_high, f_high], 0)
    bwd_a = np.concatenate([b_high, b_low], 1)
    sub = np.arange(8)[:, None]
    lane = np.arange(128)[None, :]
    point = lane % 64
    in_plane = rho[point // 8] * rho[point % 8]
    rho_c = np.zeros((2, 8, 128))
    for half in range(2):
        rho_c[half] = rho[4 * half + 2 * (sub // 4) + lane // 64]
    c = 2 * (sub // 4) + lane // 64
    parts = []
    for operator, scale in ((derivative, rho_c[0] * in_plane), (derivative.T, 1.0)):
        for sign in (1, -1):
            for swap in range(4):
                near = operator[c, c ^ swap]
                far = operator[c, 7 - (c ^ swap)]
                parts.append((near + sign * far) * 0.5 * scale)
    coeffs = np.concatenate([np.stack(parts), rho_c], 0)
    lane_in = np.arange(128)[:, None]
    lane_out = np.arange(128)[None, :]
    sides = [lane_in == lane_out % 16 * 8 + edge for edge in (0, 7)]
    pick = np.concatenate(sides, 1).astype(jnp.bfloat16)
    pick = np.concatenate([pick, pick], 0)
    wide = np.arange(TILES * 128)[None, :]
    slot = wide // 128 * 16 + wide % 128 // 8
    spread = [(lane_in == slot) & (wide % 8 == edge) for edge in (0, 7)]
    spread = np.concatenate(spread, 0).astype(jnp.bfloat16)
    tables = (fwd_a, f_low, bwd_a, b_high, coeffs.astype(np.float32), pick)
    return tuple(jnp.asarray(table) for table in tables), jnp.asarray(spread)


def split(value):
    high = value.astype(jnp.bfloat16)
    return high, (value - high.astype(jnp.float32)).astype(jnp.bfloat16)


def dot(a, b):
    return jnp.dot(a, b, preferred_element_type=jnp.float32)


def mirror(value):
    return pltpu.roll(pltpu.roll(value, 64, 1), 4, 0)


def along_z(low, high, coeffs, base):
    sums = []
    for value in (low + high, low - high):
        turned = pltpu.roll(value, 64, 1)
        variants = [value, turned, pltpu.roll(value, 4, 0), pltpu.roll(turned, 4, 0)]
        terms = [coeffs[base + k] * variants[k] for k in range(4)]
        sums.append((terms[0] + terms[1]) + (terms[2] + terms[3]))
        base += 4
    return sums[0] + sums[1], sums[1] - sums[0]


def rank_of(slab, cycle):
    if cycle & (cycle - 1) == 0:
        return slab >> (cycle.bit_length() - 1)
    return lax.div(slab, cycle)


def lanes_from(value, index):
    return jnp.take_along_axis(value, index, axis=1, mode="promise_in_bounds")


def flip(value, sub, lane):
    value = lanes_from(value, lane ^ 7)
    odd = jnp.where(sub % 2 == 0, pltpu.roll(value, 7, 0), pltpu.roll(value, 1, 0))
    return jnp.where(sub % 4 < 2, pltpu.roll(odd, 6, 0), pltpu.roll(odd, 2, 0))


def iotas():
    sub = lax.broadcasted_iota(jnp.int32, (8, 128), 0)
    lane = lax.broadcasted_iota(jnp.int32, (8, 128), 1)
    return sub, lane


def turned_flag(map_ref, row):
    return jnp.broadcast_to(map_ref[pl.ds(row, 1), 0:1], (8, 128)) != 0


def apply_kernel(
    cycle, ids_ref, dev_ref,
    u_ref, m_ref, map_ref, fa_ref, fl_ref, ba_ref, bh_ref, co_ref, pick_ref,
    out_ref, left_ref, right_ref, swap_ref,
    g_ref, fh_ref, fl2_ref, lz_ref, l_ref, face_ref, pl_ref, pr_ref,
):
    step = pl.program_id(0)
    sub, lane = iotas()
    rows = u_ref.shape[0]
    slabs = rows // 64
    u = u_ref[...].reshape(slabs * EZ, 2, 8, 128)
    v = (u * co_ref[16:18][None]).reshape(rows, 128)
    high, low = split(v)
    uk = jnp.concatenate([high, low], 1)
    g_ref[...] = dot(uk, fa_ref[...]) + dot(high, fl_ref[...])

    for e in range(slabs * EZ):
        base = e * 16
        mbase = e * 48
        low, high = along_z(
            u_ref[base : base + 8, :], mirror(u_ref[base + 8 : base + 16, :]), co_ref, 0
        )
        low = low * m_ref[mbase + 32 : mbase + 40, :]
        high = high * mirror(m_ref[mbase + 40 : mbase + 48, :])
        low, high = along_z(low, high, co_ref, 8)
        lz_ref[base : base + 8, :] = low
        lz_ref[base + 8 : base + 16, :] = mirror(high)
        fx = m_ref[mbase : mbase + 16, :] * g_ref[base : base + 16, :128]
        fy = m_ref[mbase + 16 : mbase + 32, :] * g_ref[base : base + 16, 128:]
        xh, xl = split(fx)
        yh, yl = split(fy)
        fh_ref[base : base + 16, :128] = xh
        fh_ref[base : base + 16, 128:] = yh
        fl2_ref[base : base + 16, :128] = xl
        fl2_ref[base : base + 16, 128:] = yl
    both = dot(fh_ref[...], ba_ref[...])
    l_ref[...] = both[:, :128] + both[:, 128:] + dot(fl2_ref[...], bh_ref[...]) + lz_ref[...]

    b = lane // 8 % 8
    ey = sub % 4
    after_mask = (b == 7) & (ey < 3)
    before_mask = (b == 0) & (ey > 0)
    high_c = (sub >= 4) & (lane >= 64)
    low_c = (sub < 4) & (lane < 64)
    slot = lane // 16
    slot8 = lane // 8
    for s in range(slabs):
        tiles = []
        for k in range(TILES):
            row = s * 64 + k * 8
            t = l_ref[row : row + 8, :]
            after = pltpu.roll(pltpu.roll(t, 56, 1), 7, 0)
            before = pltpu.roll(pltpu.roll(t, 72, 1), 1, 0)
            tiles.append(
                t + jnp.where(after_mask, after, 0.0) + jnp.where(before_mask, before, 0.0)
            )
        for e in range(EZ - 1):
            top = tiles[2 * e + 1]
            bottom = tiles[2 * e + 2]
            tiles[2 * e + 1] = top + jnp.where(
                high_c, pltpu.roll(pltpu.roll(bottom, 64, 1), 4, 0), 0.0
            )
            tiles[2 * e + 2] = bottom + jnp.where(
                low_c, pltpu.roll(pltpu.roll(top, 64, 1), 4, 0), 0.0
            )
        for k in range(TILES):
            row = s * 64 + k * 8
            out_ref[row : row + 8, :] = tiles[k]
        zed = jnp.where(sub < 4, tiles[0], tiles[TILES - 1])
        if s % 2 == 0:
            even = zed
        else:
            odd = pltpu.roll(zed, 64, 1)
            where = pl.ds(pl.multiple_of((step * slabs + s - 1) * 4, 8), 8)
            swap_ref[where, :] = jnp.where((sub < 4) == (lane < 64), even, odd)
    high, low = split(out_ref[...])
    face_ref[...] = dot(jnp.concatenate([high, low], 1), pick_ref[...])
    for s in range(slabs):
        row = s * 64
        left = face_ref[row : row + 8, :128]
        right = face_ref[row : row + 8, 128:]
        for k in range(1, TILES):
            row = s * 64 + k * 8
            left = jnp.where(slot == k, face_ref[row : row + 8, :128], left)
            right = jnp.where(slot == k, face_ref[row : row + 8, 128:], right)
        position = step * slabs + s
        flag = turned_flag(map_ref, position)
        right = jnp.where(flag, flip(right, sub, lane), right)
        rank = rank_of(ids_ref[dev_ref[0] + position], cycle)
        where = pl.ds(pl.multiple_of(rank * 8, 8), 8)
        left_ref[where, :] = left
        right_ref[where, :] = right
        place = rank & 15
        mask = ((slot8 == place) & (sub < 4)) | ((slot8 == ((place + 15) & 15)) & (sub >= 4))
        pl_ref[where, :] = jnp.where(mask, pltpu.roll(left, place * 8, 1), 0.0)
        pr_ref[where, :] = jnp.where(mask, pltpu.roll(right, place * 8, 1), 0.0)

    @pl.when(step == pl.num_programs(0) - 1)
    def _():
        count = pl_ref.shape[0] // 16
        base = pl_ref.shape[0] // 2
        for from_ref in (pl_ref, pr_ref):
            parts = from_ref[...].reshape(-1, 16, 8, 128)
            swap_ref[base : base + count, :] = jnp.sum(parts, axis=1).reshape(count, 128)
            base += count


def edge_kernel(left_ref, right_ref, swap_ref, left_out, right_out):
    sub, lane = iotas()
    low_edge = (sub < 4) & (lane < 8)
    high_edge = (sub >= 4) & (lane >= 120)
    slabs = left_ref.shape[0] // 8
    base = slabs * 4
    for face_ref, to_ref in ((left_ref, left_out), (right_ref, right_out)):
        for s in range(slabs):
            place = s % 16
            if place == 0:
                edge = pltpu.roll(swap_ref[base + s // 2 : base + s // 2 + 8, :], 4, 0)
            low = pltpu.roll(edge, (136 - 8 * place) % 128, 1)
            high = pltpu.roll(edge, 120 - 8 * place, 1)
            other = jnp.where(low_edge, low, jnp.where(high_edge, high, 0.0))
            to_ref[s * 8 : s * 8 + 8, :] = face_ref[s * 8 : s * 8 + 8, :] + other
        base += slabs // 2


def fix_kernel(
    cycle, total, ids_ref, dev_ref,
    in_ref, map_ref, fprev_ref, fnext_ref, zed_ref, spread_ref,
    out_ref, x_ref, y_ref,
):
    step = pl.program_id(0)
    sub, lane = iotas()
    slabs = in_ref.shape[0] // 64
    low_c = (sub < 4) & (lane < 64)
    high_c = (sub >= 4) & (lane >= 64)

    def incoming(face_ref, rank):
        return face_ref[pl.ds(pl.multiple_of(rank * 8, 8), 8), :]

    half = slabs * 8
    for s in range(slabs):
        p = step * slabs + s
        own = ids_ref[dev_ref[0] + p]
        before = jnp.where(own == 0, total - 1, own - 1)
        after = jnp.where(own == total - 1, 0, own + 1)
        left = incoming(fprev_ref, rank_of(before, cycle))
        right = incoming(fnext_ref, rank_of(after, cycle))
        right = jnp.where(turned_flag(map_ref, p), flip(right, sub, lane), right)
        x_ref[s * 8 : s * 8 + 8, :128] = left
        x_ref[s * 8 : s * 8 + 8, 128:] = right
    high, low = split(x_ref[...])
    both = dot(jnp.concatenate([high, low], 0), spread_ref[...])
    y_ref[...] = both[:half] + both[half:]
    for s in range(slabs):
        zed = pltpu.roll(zed_ref[s // 2 * 8 : s // 2 * 8 + 8, :], 4, 0)
        if s % 2 == 0:
            zed = pltpu.roll(zed, 64, 1)
        for k in range(TILES):
            row = s * 64 + k * 8
            t = in_ref[row : row + 8, :] + y_ref[s * 8 : s * 8 + 8, k * 128 : k * 128 + 128]
            if k == 0:
                t = t + jnp.where(low_c, zed, 0.0)
            if k == TILES - 1:
                t = t + jnp.where(high_c, zed, 0.0)
            out_ref[row : row + 8, :] = t


def whole_of(array):
    return pl.BlockSpec(array.shape, lambda i, *_: (0,) * array.ndim)


def apply_local(ids, dev, u, m, face_map, tables, cycle):
    slab_count = face_map.shape[0]
    steps = slab_count // BLOCK
    rows = BLOCK * 64
    f32 = jnp.float32
    shapes = [
        (slab_count * 64, 128),
        (slab_count * 8, 128),
        (slab_count * 8, 128),
        (slab_count * 5, 128),
    ]
    row_block = lambda n: pl.BlockSpec((n, 128), lambda i, *_: (i, 0))
    whole = lambda shape: pl.BlockSpec(shape, lambda i, *_: (0, 0))
    return pl.pallas_call(
        functools.partial(apply_kernel, cycle),
        grid_spec=pltpu.PrefetchScalarGridSpec(
            num_scalar_prefetch=2,
            grid=(steps,),
            in_specs=[row_block(rows), row_block(rows * 3), whole((slab_count, 128))]
            + [whole_of(t) for t in tables],
            out_specs=[
                row_block(rows),
                whole(shapes[1]),
                whole(shapes[2]),
                whole(shapes[3]),
            ],
            scratch_shapes=[
                pltpu.VMEM((rows, 256), f32),
                pltpu.VMEM((rows, 256), jnp.bfloat16),
                pltpu.VMEM((rows, 256), jnp.bfloat16),
                pltpu.VMEM((rows, 128), f32),
                pltpu.VMEM((rows, 128), f32),
                pltpu.VMEM((rows, 256), f32),
                pltpu.VMEM(shapes[1], f32),
                pltpu.VMEM(shapes[1], f32),
            ],
        ),
        out_shape=[jax.ShapeDtypeStruct(s, f32) for s in shapes],
        name="apply_local",
    )(ids, dev, u, m, face_map, *tables)


def add_edges(left, right, swap):
    return pl.pallas_call(
        edge_kernel,
        out_shape=[jax.ShapeDtypeStruct(left.shape, jnp.float32)] * 2,
        name="add_edges",
    )(left, right, swap)


def fix_faces(ids, dev, local, face_map, fprev, fnext, zed, spread, cycle):
    slab_count = face_map.shape[0]
    steps = slab_count // FIX_BLOCK
    rows = FIX_BLOCK * 64
    return pl.pallas_call(
        functools.partial(fix_kernel, cycle, slab_count * cycle),
        grid_spec=pltpu.PrefetchScalarGridSpec(
            num_scalar_prefetch=2,
            grid=(steps,),
            in_specs=[
                pl.BlockSpec((rows, 128), lambda i, *_: (i, 0)),
                pl.BlockSpec((slab_count, 128), lambda i, *_: (0, 0)),
                whole_of(fprev),
                whole_of(fnext),
                pl.BlockSpec((FIX_BLOCK * 4, 128), lambda i, *_: (i, 0)),
                whole_of(spread),
            ],
            out_specs=pl.BlockSpec((rows, 128), lambda i, *_: (i, 0)),
            scratch_shapes=[
                pltpu.VMEM((FIX_BLOCK * 8, 256), jnp.float32),
                pltpu.VMEM((FIX_BLOCK * 8, TILES * 128), jnp.float32),
            ],
        ),
        out_shape=jax.ShapeDtypeStruct(local.shape, jnp.float32),
        name="fix_faces",
    )(ids, dev, local, face_map, fprev, fnext, zed, spread)


def send(value, by, across):
    slabs = lax.axis_size("slab")
    layers = lax.axis_size("layer")
    pairs = [
        (s * layers + l, (s + by) % slabs * layers + (l + across) % layers)
        for s in range(slabs)
        for l in range(layers)
    ]
    return lax.ppermute(value, ("slab", "layer"), pairs)


def body(nodal_field, metric, slab_ids, face_map):
    slab_count = nodal_field.shape[1]
    cycle_size = lax.axis_size("slab")
    first = lax.axis_index("slab").reshape(1) * slab_count
    tables, spread = kernel_tables()
    u = nodal_field.reshape(slab_count, EZ, EY, 4, 128).transpose(0, 1, 3, 2, 4)
    u = u.reshape(slab_count * 64, 128)
    m = metric.reshape(slab_count, EZ, EY, 3, 4, 128).transpose(0, 1, 3, 4, 2, 5)
    m = m.reshape(slab_count * 192, 128)
    local, left, right, swap = apply_local(
        slab_ids, first, u, m, face_map, tables, cycle_size
    )
    swap = send(swap, 0, 1)
    left, right = add_edges(left, right, swap)
    fprev = send(right, 1, 0)
    fnext = send(left, -1, 0)
    out = fix_faces(
        slab_ids, first, local, face_map, fprev, fnext, swap, spread, cycle_size
    )
    out = out.reshape(slab_count, EZ, 4, EY, 128).transpose(0, 1, 3, 2, 4)
    return out.reshape(1, slab_count, EZ, EY, PTS)


def solution(mesh):
    return jax.shard_map(
        body,
        mesh=mesh,
        in_specs=(
            P("layer", "slab", None, None, None),
            P("layer", "slab", None, None, None, None),
            P(),
            P("slab", None),
        ),
        out_specs=P("layer", "slab", None, None, None),
        check_vma=False,
    )
```

```python
import functools

import jax
import jax.numpy as jnp
import numpy as np
from jax import lax
from jax.experimental import pallas as pl
from jax.experimental.pallas import tpu as pltpu
from jax.sharding import PartitionSpec as P

P_SIZE = 8
PTS = 512
EY = 4
EZ = 4
TILES = EZ * 2
BLOCK = 8
FIX_BLOCK = 8


def legendre_pair(gll_nodes, degree):
    lower_poly = gll_nodes * 0.0 + 1.0
    upper_poly = gll_nodes.copy()
    for poly_order in range(2, degree + 1):
        lower_poly, upper_poly = (
            upper_poly,
            ((2 * poly_order - 1) * gll_nodes * upper_poly - (poly_order - 1) * lower_poly)
            / poly_order,
        )
    return (lower_poly, upper_poly)


def gll_tables():
    degree = P_SIZE - 1
    gll_nodes = -np.cos(np.pi * np.arange(P_SIZE) / degree)
    for newton_sweep in range(100):
        lower_poly, upper_poly = legendre_pair(gll_nodes, degree)
        gll_nodes = gll_nodes - (gll_nodes * upper_poly - lower_poly) / ((degree + 1) * upper_poly)
    lower_poly, upper_poly = legendre_pair(gll_nodes, degree)
    quad_weights = 2.0 / (degree * (degree + 1) * upper_poly * upper_poly)
    identity = np.eye(P_SIZE)
    differ = gll_nodes[:, None] - gll_nodes[None, :] + identity
    derivative = upper_poly[:, None] / (upper_poly[None, :] * differ)
    derivative = derivative * (1.0 - identity)
    derivative[0, 0] = -degree * (degree + 1) / 4.0
    derivative[degree, degree] = degree * (degree + 1) / 4.0
    return derivative, quad_weights


def split_table(table):
    high = table.astype(np.float32).astype(jnp.bfloat16)
    low = (table - high.astype(np.float64)).astype(np.float32).astype(jnp.bfloat16)
    return high, low


def kernel_tables():
    derivative, rho = gll_tables()
    two = np.eye(2)
    eye = np.eye(P_SIZE)
    plane = np.tile(np.kron(rho, rho), 2)
    along_x = np.kron(two, np.kron(eye, derivative))
    along_y = np.kron(two, np.kron(derivative, eye))
    forward = np.concatenate([along_x.T * plane[None, :], along_y.T * plane[None, :]], 1)
    backward = np.concatenate([along_x, along_y], 0)
    f_high, f_low = split_table(forward)
    b_high, b_low = split_table(backward)
    fwd_a = np.concatenate([f_high, f_high], 0)
    bwd_a = np.concatenate([b_high, b_low], 1)
    sub = np.arange(8)[:, None]
    lane = np.arange(128)[None, :]
    point = lane % 64
    in_plane = rho[point // 8] * rho[point % 8]
    rho_c = np.zeros((2, 8, 128))
    for half in range(2):
        rho_c[half] = rho[4 * half + 2 * (sub // 4) + lane // 64]
    c = 2 * (sub // 4) + lane // 64
    parts = []
    for operator, scale in ((derivative, rho_c[0] * in_plane), (derivative.T, 1.0)):
        for sign in (1, -1):
            for swap in range(4):
                near = operator[c, c ^ swap]
                far = operator[c, 7 - (c ^ swap)]
                parts.append((near + sign * far) * 0.5 * scale)
    coeffs = np.concatenate([np.stack(parts), rho_c], 0)
    lane_in = np.arange(128)[:, None]
    lane_out = np.arange(128)[None, :]
    sides = [lane_in == lane_out % 16 * 8 + edge for edge in (0, 7)]
    pick = np.concatenate(sides, 1).astype(jnp.bfloat16)
    pick = np.concatenate([pick, pick], 0)
    wide = np.arange(TILES * 128)[None, :]
    slot = wide // 128 * 16 + wide % 128 // 8
    spread = [(lane_in == slot) & (wide % 8 == edge) for edge in (0, 7)]
    spread = np.concatenate(spread, 0).astype(jnp.bfloat16)
    tables = (fwd_a, f_low, bwd_a, b_high, coeffs.astype(np.float32), pick)
    return tuple(jnp.asarray(table) for table in tables), jnp.asarray(spread)


def split(value):
    high = value.astype(jnp.bfloat16)
    return high, (value - high.astype(jnp.float32)).astype(jnp.bfloat16)


def dot(a, b):
    return jnp.dot(a, b, preferred_element_type=jnp.float32)


def mirror(value):
    return pltpu.roll(pltpu.roll(value, 64, 1), 4, 0)


def along_z(low, high, coeffs, base):
    sums = []
    for value in (low + high, low - high):
        turned = pltpu.roll(value, 64, 1)
        variants = [value, turned, pltpu.roll(value, 4, 0), pltpu.roll(turned, 4, 0)]
        terms = [coeffs[base + k] * variants[k] for k in range(4)]
        sums.append((terms[0] + terms[1]) + (terms[2] + terms[3]))
        base += 4
    return sums[0] + sums[1], sums[1] - sums[0]


def rank_of(slab, cycle):
    if cycle & (cycle - 1) == 0:
        return slab >> (cycle.bit_length() - 1)
    return lax.div(slab, cycle)


def lanes_from(value, index):
    return jnp.take_along_axis(value, index, axis=1, mode="promise_in_bounds")


def flip(value, sub, lane):
    value = lanes_from(value, lane ^ 7)
    odd = jnp.where(sub % 2 == 0, pltpu.roll(value, 7, 0), pltpu.roll(value, 1, 0))
    return jnp.where(sub % 4 < 2, pltpu.roll(odd, 6, 0), pltpu.roll(odd, 2, 0))


def iotas():
    sub = lax.broadcasted_iota(jnp.int32, (8, 128), 0)
    lane = lax.broadcasted_iota(jnp.int32, (8, 128), 1)
    return sub, lane


def turned_flag(map_ref, row):
    return jnp.broadcast_to(map_ref[pl.ds(row, 1), 0:1], (8, 128)) != 0


def apply_kernel(
    cycle, ids_ref, dev_ref,
    u_ref, m_ref, map_ref, fa_ref, fl_ref, ba_ref, bh_ref, co_ref, pick_ref,
    out_ref, left_ref, right_ref, zed_ref, el_ref, er_ref,
    g_ref, fh_ref, fl2_ref, lz_ref, l_ref, face_ref, pl_ref, pr_ref,
):
    step = pl.program_id(0)
    sub, lane = iotas()
    rows = u_ref.shape[0]
    slabs = rows // 64
    u = u_ref[...].reshape(slabs * EZ, 2, 8, 128)
    v = (u * co_ref[16:18][None]).reshape(rows, 128)
    high, low = split(v)
    uk = jnp.concatenate([high, low], 1)
    g_ref[...] = dot(uk, fa_ref[...]) + dot(high, fl_ref[...])

    for e in range(slabs * EZ):
        base = e * 16
        mbase = e * 48
        low, high = along_z(
            u_ref[base : base + 8, :], mirror(u_ref[base + 8 : base + 16, :]), co_ref, 0
        )
        low = low * m_ref[mbase + 32 : mbase + 40, :]
        high = high * mirror(m_ref[mbase + 40 : mbase + 48, :])
        low, high = along_z(low, high, co_ref, 8)
        lz_ref[base : base + 8, :] = low
        lz_ref[base + 8 : base + 16, :] = mirror(high)
        fx = m_ref[mbase : mbase + 16, :] * g_ref[base : base + 16, :128]
        fy = m_ref[mbase + 16 : mbase + 32, :] * g_ref[base : base + 16, 128:]
        xh, xl = split(fx)
        yh, yl = split(fy)
        fh_ref[base : base + 16, :128] = xh
        fh_ref[base : base + 16, 128:] = yh
        fl2_ref[base : base + 16, :128] = xl
        fl2_ref[base : base + 16, 128:] = yl
    both = dot(fh_ref[...], ba_ref[...])
    l_ref[...] = both[:, :128] + both[:, 128:] + dot(fl2_ref[...], bh_ref[...]) + lz_ref[...]

    b = lane // 8 % 8
    ey = sub % 4
    after_mask = (b == 7) & (ey < 3)
    before_mask = (b == 0) & (ey > 0)
    high_c = (sub >= 4) & (lane >= 64)
    low_c = (sub < 4) & (lane < 64)
    slot = lane // 16
    slot8 = lane // 8
    for s in range(slabs):
        tiles = []
        for k in range(TILES):
            row = s * 64 + k * 8
            t = l_ref[row : row + 8, :]
            after = pltpu.roll(pltpu.roll(t, 56, 1), 7, 0)
            before = pltpu.roll(pltpu.roll(t, 72, 1), 1, 0)
            tiles.append(
                t + jnp.where(after_mask, after, 0.0) + jnp.where(before_mask, before, 0.0)
            )
        for e in range(EZ - 1):
            top = tiles[2 * e + 1]
            bottom = tiles[2 * e + 2]
            tiles[2 * e + 1] = top + jnp.where(
                high_c, pltpu.roll(pltpu.roll(bottom, 64, 1), 4, 0), 0.0
            )
            tiles[2 * e + 2] = bottom + jnp.where(
                low_c, pltpu.roll(pltpu.roll(top, 64, 1), 4, 0), 0.0
            )
        for k in range(TILES):
            row = s * 64 + k * 8
            out_ref[row : row + 8, :] = tiles[k]
        zed = jnp.where(sub < 4, tiles[0], tiles[TILES - 1])
        if s % 2 == 0:
            even = zed
        else:
            odd = pltpu.roll(zed, 64, 1)
            zed_ref[s // 2 * 8 : s // 2 * 8 + 8, :] = jnp.where(
                (sub < 4) == (lane < 64), even, odd
            )
    high, low = split(out_ref[...])
    face_ref[...] = dot(jnp.concatenate([high, low], 1), pick_ref[...])
    for s in range(slabs):
        row = s * 64
        left = face_ref[row : row + 8, :128]
        right = face_ref[row : row + 8, 128:]
        for k in range(1, TILES):
            row = s * 64 + k * 8
            left = jnp.where(slot == k, face_ref[row : row + 8, :128], left)
            right = jnp.where(slot == k, face_ref[row : row + 8, 128:], right)
        position = step * slabs + s
        flag = turned_flag(map_ref, position)
        right = jnp.where(flag, flip(right, sub, lane), right)
        rank = rank_of(ids_ref[dev_ref[0] + position], cycle)
        where = pl.ds(pl.multiple_of(rank * 8, 8), 8)
        left_ref[where, :] = left
        right_ref[where, :] = right
        place = rank & 15
        mask = ((slot8 == place) & (sub < 4)) | ((slot8 == ((place + 15) & 15)) & (sub >= 4))
        pl_ref[where, :] = jnp.where(mask, pltpu.roll(left, place * 8, 1), 0.0)
        pr_ref[where, :] = jnp.where(mask, pltpu.roll(right, place * 8, 1), 0.0)

    @pl.when(step == pl.num_programs(0) - 1)
    def _():
        for from_ref, to_ref in ((pl_ref, el_ref), (pr_ref, er_ref)):
            parts = from_ref[...].reshape(-1, 16, 8, 128)
            to_ref[...] = jnp.sum(parts, axis=1).reshape(to_ref.shape)


def fix_kernel(
    cycle, total, ids_ref, dev_ref,
    in_ref, map_ref, fprev_ref, fnext_ref, zed_ref, eprev_ref, enext_ref, spread_ref,
    out_ref, x_ref, y_ref,
):
    step = pl.program_id(0)
    sub, lane = iotas()
    slabs = in_ref.shape[0] // 64
    low_c = (sub < 4) & (lane < 64)
    high_c = (sub >= 4) & (lane >= 64)
    low_edge = (sub < 4) & (lane < 8)
    high_edge = (sub >= 4) & (lane >= 120)

    def incoming(face_ref, edge_ref, j):
        face = face_ref[pl.ds(pl.multiple_of(j * 8, 8), 8), :]
        edge = edge_ref[pl.ds(pl.multiple_of((j >> 4) * 8, 8), 8), :]
        shift = ((16 - (j & 15)) & 15) * 8
        edge = pltpu.roll(pltpu.roll(edge, shift, 1), 4, 0)
        edge = jnp.where(
            low_edge,
            pltpu.roll(edge, 8, 1),
            jnp.where(high_edge, pltpu.roll(edge, 120, 1), 0.0),
        )
        return face + edge

    half = slabs * 8
    for s in range(slabs):
        p = step * slabs + s
        own = ids_ref[dev_ref[0] + p]
        before = jnp.where(own == 0, total - 1, own - 1)
        after = jnp.where(own == total - 1, 0, own + 1)
        left = incoming(fprev_ref, eprev_ref, rank_of(before, cycle))
        right = incoming(fnext_ref, enext_ref, rank_of(after, cycle))
        right = jnp.where(turned_flag(map_ref, p), flip(right, sub, lane), right)
        x_ref[s * 8 : s * 8 + 8, :128] = left
        x_ref[s * 8 : s * 8 + 8, 128:] = right
    high, low = split(x_ref[...])
    both = dot(jnp.concatenate([high, low], 0), spread_ref[...])
    y_ref[...] = both[:half] + both[half:]
    for s in range(slabs):
        zed = pltpu.roll(zed_ref[s // 2 * 8 : s // 2 * 8 + 8, :], 4, 0)
        if s % 2 == 0:
            zed = pltpu.roll(zed, 64, 1)
        for k in range(TILES):
            row = s * 64 + k * 8
            t = in_ref[row : row + 8, :] + y_ref[s * 8 : s * 8 + 8, k * 128 : k * 128 + 128]
            if k == 0:
                t = t + jnp.where(low_c, zed, 0.0)
            if k == TILES - 1:
                t = t + jnp.where(high_c, zed, 0.0)
            out_ref[row : row + 8, :] = t


def whole_of(array):
    return pl.BlockSpec(array.shape, lambda i, *_: (0,) * array.ndim)


def apply_local(ids, dev, u, m, face_map, tables, cycle):
    slab_count = face_map.shape[0]
    steps = slab_count // BLOCK
    rows = BLOCK * 64
    f32 = jnp.float32
    shapes = [
        (slab_count * 64, 128),
        (slab_count * 8, 128),
        (slab_count * 8, 128),
        (slab_count * 4, 128),
        (slab_count // 2, 128),
        (slab_count // 2, 128),
    ]
    row_block = lambda n: pl.BlockSpec((n, 128), lambda i, *_: (i, 0))
    whole = lambda shape: pl.BlockSpec(shape, lambda i, *_: (0, 0))
    return pl.pallas_call(
        functools.partial(apply_kernel, cycle),
        grid_spec=pltpu.PrefetchScalarGridSpec(
            num_scalar_prefetch=2,
            grid=(steps,),
            in_specs=[row_block(rows), row_block(rows * 3), whole((slab_count, 128))]
            + [whole_of(t) for t in tables],
            out_specs=[
                row_block(rows),
                whole(shapes[1]),
                whole(shapes[2]),
                row_block(BLOCK * 4),
                whole(shapes[4]),
                whole(shapes[5]),
            ],
            scratch_shapes=[
                pltpu.VMEM((rows, 256), f32),
                pltpu.VMEM((rows, 256), jnp.bfloat16),
                pltpu.VMEM((rows, 256), jnp.bfloat16),
                pltpu.VMEM((rows, 128), f32),
                pltpu.VMEM((rows, 128), f32),
                pltpu.VMEM((rows, 256), f32),
                pltpu.VMEM(shapes[1], f32),
                pltpu.VMEM(shapes[1], f32),
            ],
        ),
        out_shape=[jax.ShapeDtypeStruct(s, f32) for s in shapes],
        name="apply_local",
    )(ids, dev, u, m, face_map, *tables)


def fix_faces(ids, dev, local, face_map, fprev, fnext, zed, eprev, enext, spread, cycle):
    slab_count = face_map.shape[0]
    steps = slab_count // FIX_BLOCK
    rows = FIX_BLOCK * 64
    return pl.pallas_call(
        functools.partial(fix_kernel, cycle, slab_count * cycle),
        grid_spec=pltpu.PrefetchScalarGridSpec(
            num_scalar_prefetch=2,
            grid=(steps,),
            in_specs=[
                pl.BlockSpec((rows, 128), lambda i, *_: (i, 0)),
                pl.BlockSpec((slab_count, 128), lambda i, *_: (0, 0)),
                whole_of(fprev),
                whole_of(fnext),
                pl.BlockSpec((FIX_BLOCK * 4, 128), lambda i, *_: (i, 0)),
                whole_of(eprev),
                whole_of(enext),
                whole_of(spread),
            ],
            out_specs=pl.BlockSpec((rows, 128), lambda i, *_: (i, 0)),
            scratch_shapes=[
                pltpu.VMEM((FIX_BLOCK * 8, 256), jnp.float32),
                pltpu.VMEM((FIX_BLOCK * 8, TILES * 128), jnp.float32),
            ],
        ),
        out_shape=jax.ShapeDtypeStruct(local.shape, jnp.float32),
        name="fix_faces",
    )(ids, dev, local, face_map, fprev, fnext, zed, eprev, enext, spread)


def send(value, by, across):
    slabs = lax.axis_size("slab")
    layers = lax.axis_size("layer")
    pairs = [
        (s * layers + l, (s + by) % slabs * layers + (l + across) % layers)
        for s in range(slabs)
        for l in range(layers)
    ]
    return lax.ppermute(value, ("slab", "layer"), pairs)


def body(nodal_field, metric, slab_ids, face_map):
    slab_count = nodal_field.shape[1]
    cycle_size = lax.axis_size("slab")
    first = lax.axis_index("slab").reshape(1) * slab_count
    tables, spread = kernel_tables()
    u = nodal_field.reshape(slab_count, EZ, EY, 4, 128).transpose(0, 1, 3, 2, 4)
    u = u.reshape(slab_count * 64, 128)
    m = metric.reshape(slab_count, EZ, EY, 3, 4, 128).transpose(0, 1, 3, 4, 2, 5)
    m = m.reshape(slab_count * 192, 128)
    local, left, right, zed, edge_left, edge_right = apply_local(
        slab_ids, first, u, m, face_map, tables, cycle_size
    )
    zed = send(zed, 0, 1)
    fprev = send(right, 1, 0)
    fnext = send(left, -1, 0)
    eprev = send(edge_right, 1, 1)
    enext = send(edge_left, -1, 1)

    out = fix_faces(
        slab_ids, first, local, face_map, fprev, fnext, zed, eprev, enext, spread, cycle_size
    )
    out = out.reshape(slab_count, EZ, 4, EY, 128).transpose(0, 1, 3, 2, 4)
    return out.reshape(1, slab_count, EZ, EY, PTS)


def solution(mesh):
    return jax.shard_map(
        body,
        mesh=mesh,
        in_specs=(
            P("layer", "slab", None, None, None),
            P("layer", "slab", None, None, None, None),
            P(),
            P("slab", None),
        ),
        out_specs=P("layer", "slab", None, None, None),
        check_vma=False,
    )
```
